512 devices in a mesh: gz: 128 (over y_lo, z, x), gy: 4 (over y_hi, core).
Axes of the slice: x: 4, y: 8 (y_hi: 2, y_lo: 4; y = y_hi * 4 + y_lo), z: 8, core: 2. Of those that a mesh axis runs over, the one named last changes fastest.
Arguments:
- volume: bfloat16 [512, 16, 32, 128], P('gz', 'gy'), may hold values from -6 to 6
- kernel_a: bfloat16 [3, 3, 3, 128, 128], replicated, may hold values from -0.109375 to 0.109375
- bias_a: float32 [128], replicated, may hold values from -3 to 3
- kernel_b: bfloat16 [3, 3, 3, 128, 256], P(None, None, None, None, 'gy'), may hold values from -0.109375 to 0.109375
- bias_b: float32 [256], P('gy'), may hold values from -3 to 3
- kernel_c: bfloat16 [3, 3, 3, 256, 512], P(None, None, None, None, 'gy'), may hold values from -0.078125 to 0.078125
- bias_c: float32 [512], P('gy'), may hold values from -3 to 3
Outputs:
- skip_a: bfloat16 [512, 16, 32, 128], P('gz', 'gy')
- skip_b: bfloat16 [256, 8, 16, 256], P('gz', None, None, 'gy')
- bottom: bfloat16 [128, 4, 8, 512], P('gz', None, None, 'gy')
The draws below stay inside these ranges and needn't reach their ends.
All inputs are finite; a program needn't handle non-finite values.
Results may differ from the reference program's by a relative error of at most 0.0054.
Values may be sent and summed in bfloat16 or wider, within the bound.
No kernel may reach another device: no remote copies, remote signals or barrier semaphores. Data moves between devices by JAX's collectives and lax.ppermute only.
A program may use at most 64 MiB of HBM per device.

```python
import jax
import jax.numpy as jnp
from jax import lax

CA = 128
CB = 256
CC = 512
XW = 32
DA = 512
HA = 16


def block_scale(key, dims, shards, least, largest):
    def one(position, parts):
        heights = jax.random.uniform(jax.random.fold_in(jax.random.fold_in(key, 6), position), (parts,), jnp.float32, least / len(shards), largest / len(shards))
        return jnp.repeat(jnp.exp(heights), dims[position] // parts).reshape((-1,) + (1,) * (len(dims) - position - 1))

    loudness = one(*shards[0])
    for cut in shards[1:]:
        loudness = loudness * one(*cut)
    return loudness


def normal_values(rng, dims, scale, most, cuts=(), dtype=jnp.bfloat16):
    entries = jax.random.normal(rng, dims, jnp.float32) * scale
    if len(cuts) > 0:
        entries = block_scale(rng, dims, cuts, -0.22, 0.18) * entries
    return jnp.clip(entries, min=-most, max=most).astype(dtype)


def setup_inputs(seed: int = 0) -> dict:
    key_of = jax.random.split(jax.random.key(seed), 8)
    return {
        "volume": normal_values(key_of[0], (DA, HA, XW, CA), 1.0, 6.0, ((0, 128), (1, 4))),
        "kernel_a": normal_values(key_of[1], (3, 3, 3, CA, CA), (27 * CA) ** -0.5, 0.109375),
        "bias_a": normal_values(key_of[2], (CA,), 0.5, 3.0, (), jnp.float32),
        "kernel_b": normal_values(key_of[3], (3, 3, 3, CA, CB), (27 * CA) ** -0.5, 0.109375, ((4, 4),)),
        "bias_b": normal_values(key_of[4], (CB,), 0.5, 3.0, ((0, 4),), jnp.float32),
        "kernel_c": normal_values(key_of[5], (3, 3, 3, CB, CC), (27 * CB) ** -0.5, 0.078125, ((4, 4),)),
        "bias_c": normal_values(key_of[6], (CC,), 0.5, 3.0, ((0, 4),), jnp.float32),
    }


def conv_relu(field, kernel, bias):
    out = lax.conv_general_dilated(field[None], kernel, (1, 1, 1), ((1, 1), (1, 1), (1, 1)), dimension_numbers=("NDHWC", "DHWIO", "NDHWC"), preferred_element_type=jnp.float32)[0]
    return jnp.maximum(out + bias.astype(jnp.float32), 0.0).astype(jnp.bfloat16)


def shrink(field):
    depth, height, width, chans = field.shape
    blocks = field.reshape(depth // 2, 2, height // 2, 2, width // 2, 2, chans)
    return jnp.max(blocks, axis=(1, 3, 5))


def reference(volume, kernel_a, bias_a, kernel_b, bias_b, kernel_c, bias_c):
    skip_a = conv_relu(volume, kernel_a, bias_a)
    skip_b = conv_relu(shrink(skip_a), kernel_b, bias_b)
    bottom = conv_relu(shrink(skip_b), kernel_c, bias_c)
    return skip_a, skip_b, bottom
```

```python
import jax
import jax.numpy as jnp
from jax import lax
from jax.sharding import PartitionSpec as P


def even_groups(peers):
    return [[i, i + 1] for i in range(0, peers, 2)]


def odd_pairs(peers):
    pairs = [(i, i + 1) for i in range(1, peers - 1, 2)]
    return pairs + [(j, i) for i, j in pairs]


def swapped(field, axis, dim, width):
    peers, length = lax.axis_size(axis), field.shape[dim]
    odd = lax.axis_index(axis) % 2
    room = length - width
    outward = lax.dynamic_slice_in_dim(field, odd * room, width, dim)
    inward = lax.dynamic_slice_in_dim(field, (1 - odd) * room, width, dim)
    across = lax.ppermute(outward, axis, odd_pairs(peers))
    pair = lax.all_gather(inward, axis, axis_index_groups=even_groups(peers))
    partner = lax.dynamic_index_in_dim(pair, 1 - odd, 0, keepdims=False)
    before = jnp.where(odd == 1, partner, across)
    after = jnp.where(odd == 1, across, partner)
    return jnp.concatenate([before, field, after], axis=dim)


def conv_relu(padded, kernel, bias):
    out = lax.conv_general_dilated(
        padded[None],
        kernel,
        (1, 1, 1),
        ((0, 0), (0, 0), (1, 1)),
        dimension_numbers=("NDHWC", "DHWIO", "NDHWC"),
        preferred_element_type=jnp.float32,
    )[0]
    return jnp.maximum(out + bias, 0.0).astype(jnp.bfloat16)


def shrink(field):
    depth, height, width, chans = field.shape
    blocks = field.reshape(depth // 2, 2, height // 2, 2, width // 2, 2, chans)
    return jnp.max(blocks, axis=(1, 3, 5))


def pad_height(field):
    return jnp.pad(field, ((0, 0), (1, 1), (0, 0), (0, 0)))


def on_device(volume, kernel_a, bias_a, kernel_b, bias_b, kernel_c, bias_c):
    gz, last = lax.axis_index("gz"), lax.axis_size("gz") - 1
    wide = swapped(volume, "gz", 0, 3)
    padded = swapped(wide, "gy", 1, 1)
    full_a = conv_relu(padded, kernel_a, bias_a)
    skip_a = full_a[2:6]
    pooled_a = shrink(full_a)
    layer = lax.broadcasted_iota(jnp.int32, (4, 1, 1, 1), 0)
    outside = ((gz == 0) & (layer == 0)) | ((gz == last) & (layer == 3))
    pooled_a = jnp.where(outside, jnp.bfloat16(0), pooled_a)
    ready_b = lax.all_gather(pooled_a, "gy", axis=1, tiled=True)
    skip_b = conv_relu(pad_height(ready_b), kernel_b, bias_b)
    pooled_b = swapped(shrink(skip_b), "gz", 0, 1)
    ready_c = lax.all_gather(pooled_b, "gy", axis=3, tiled=True)
    bottom = conv_relu(pad_height(ready_c), kernel_c, bias_c)
    return (skip_a, skip_b, bottom)


def solution(mesh):
    return jax.shard_map(
        on_device,
        mesh=mesh,
        in_specs=(
            P("gz", "gy", None, None),
            P(),
            P(),
            P(None, None, None, None, "gy"),
            P("gy"),
            P(None, None, None, None, "gy"),
            P("gy"),
        ),
        out_specs=(P("gz", "gy", None, None), P("gz", None, None, "gy"), P("gz", None, None, "gy")),
        check_vma=False,
    )
```

```python
import jax
import jax.numpy as jnp
from jax import lax
from jax.sharding import PartitionSpec as P


def even_groups(peers):
    return [[i, i + 1] for i in range(0, peers, 2)]


def odd_pairs(peers):
    pairs = [(i, i + 1) for i in range(1, peers - 1, 2)]
    return pairs + [(j, i) for i, j in pairs]


def swapped(field, axis, dim, width):
    peers, length = lax.axis_size(axis), field.shape[dim]
    odd = lax.axis_index(axis) % 2
    room = length - width
    outward = lax.dynamic_slice_in_dim(field, odd * room, width, dim)
    inward = lax.dynamic_slice_in_dim(field, (1 - odd) * room, width, dim)
    across = lax.ppermute(outward, axis, odd_pairs(peers))
    pair = lax.all_gather(inward, axis, axis_index_groups=even_groups(peers))
    partner = lax.dynamic_index_in_dim(pair, 1 - odd, 0, keepdims=False)
    before = jnp.where(odd == 1, partner, across)
    after = jnp.where(odd == 1, across, partner)
    return jnp.concatenate([before, field, after], axis=dim)


def conv_relu(padded, kernel, bias):
    out = lax.conv_general_dilated(
        padded[None],
        kernel,
        (1, 1, 1),
        ((0, 0), (0, 0), (1, 1)),
        dimension_numbers=("NDHWC", "DHWIO", "NDHWC"),
        preferred_element_type=jnp.float32,
    )[0]
    return jnp.maximum(out + bias, 0.0).astype(jnp.bfloat16)


def shrink(field):
    depth, height, width, chans = field.shape
    blocks = field.reshape(depth // 2, 2, height // 2, 2, width // 2, 2, chans)
    return jnp.max(blocks, axis=(1, 3, 5))


def pad_height(field):
    return jnp.pad(field, ((0, 0), (1, 1), (0, 0), (0, 0)))


def levels(volume, kernel_a, bias_a, kernel_b, bias_b, kernel_c, bias_c):
    gz, last = lax.axis_index("gz"), lax.axis_size("gz") - 1
    wide = swapped(volume, "gz", 0, 3)
    padded = swapped(wide, "gy", 1, 1)
    full_a = conv_relu(padded, kernel_a, bias_a)
    skip_a = full_a[2:6]
    pooled_a = shrink(full_a)
    layer = lax.broadcasted_iota(jnp.int32, (4, 1, 1, 1), 0)
    outside = ((gz == 0) & (layer == 0)) | ((gz == last) & (layer == 3))
    pooled_a = jnp.where(outside, jnp.bfloat16(0), pooled_a)
    ready_b = lax.all_gather(pooled_a, "gy", axis=1, tiled=True)
    skip_b = conv_relu(pad_height(ready_b), kernel_b, bias_b)
    pooled_b = swapped(shrink(skip_b), "gz", 0, 1)
    shards = lax.all_gather(pooled_b, "gy")
    ready_c = jnp.moveaxis(shards, 0, 3).reshape(3, 4, 8, -1)
    bottom = conv_relu(pad_height(ready_c), kernel_c, bias_c)
    return (skip_a, skip_b, bottom)


def solution(mesh):
    return jax.shard_map(
        levels,
        mesh=mesh,
        in_specs=(
            P("gz", "gy", None, None),
            P(),
            P(),
            P(None, None, None, None, "gy"),
            P("gy"),
            P(None, None, None, None, "gy"),
            P("gy"),
        ),
        out_specs=(P("gz", "gy", None, None), P("gz", None, None, "gy"), P("gz", None, None, "gy")),
        check_vma=False,
    )
```

```python
import jax
import jax.numpy as jnp
from jax import lax
from jax.experimental import pallas as pl
from jax.experimental.pallas import tpu as pltpu
from jax.sharding import PartitionSpec as P

BF16, F32 = jnp.bfloat16, jnp.float32


def even_groups(peers):
    return [[i, i + 1] for i in range(0, peers, 2)]


def odd_pairs(peers):
    pairs = [(i, i + 1) for i in range(1, peers - 1, 2)]
    return pairs + [(j, i) for i, j in pairs]


def swap(outward, inward, axis):
    peers = lax.axis_size(axis)
    across = lax.ppermute(outward, axis, odd_pairs(peers))
    pair = lax.all_gather(inward, axis, axis_index_groups=even_groups(peers))
    return pair, across


def ends(field, axis, width):
    odd = lax.axis_index(axis) % 2
    room = field.shape[0] - width
    outward = lax.dynamic_slice_in_dim(field, odd * room, width, 0)
    inward = lax.dynamic_slice_in_dim(field, (1 - odd) * room, width, 0)
    return outward, inward


def local(body, inputs, outs, scratch=(), flops=0):
    spec = pl.BlockSpec(memory_space=pltpu.VMEM)
    return pl.pallas_call(
        body,
        out_shape=[jax.ShapeDtypeStruct(shape, BF16) for shape in outs],
        in_specs=[spec] * len(inputs),
        out_specs=[spec] * len(outs),
        scratch_shapes=[pltpu.VMEM(shape, dtype) for shape, dtype in scratch],
        cost_estimate=pl.CostEstimate(flops=flops, bytes_accessed=1 << 20, transcendentals=0),
        compiler_params=pltpu.CompilerParams(vmem_limit_bytes=32 << 20),
    )(*inputs)


def three_taps(wide, width, chans):
    cells = wide.shape[0]
    column = lax.broadcasted_iota(jnp.int32, (cells, chans), 0) % width
    left = jnp.where(column == 0, 0.0, pltpu.roll(wide[:, :chans], 1, 0))
    right = jnp.where(column == width - 1, 0.0, pltpu.roll(wide[:, 2 * chans :], cells - 1, 0))
    return left + wide[:, chans : 2 * chans] + right


TAPS = [(i, j) for i in range(3) for j in range(3)]


def join(volume, pair, across, wide, outward, inward):
    odd, core = lax.axis_index("gz") % 2, lax.axis_index("gy") % 2
    wide[3:7] = volume[...]
    wide[pl.ds(7 * (1 - odd), 3)] = pair[1 - odd]
    wide[pl.ds(7 * odd, 3)] = across[...]
    outward[...] = wide[:, 3 * core]
    inward[...] = wide[:, 3 * (1 - core)]


def level_a(wide, pair, across, kernel, bias, skip, pooled, x, most):
    core = lax.axis_index("gy") % 2
    x[:, 1:5] = wide[...]
    x[:, 5 * (1 - core)] = pair[1 - core]
    x[:, 5 * core] = across[...]
    weights = jnp.concatenate(
        [jnp.concatenate([kernel[i, j, tap] for tap in range(3)], axis=1) for i, j in TAPS], axis=0
    )
    for p in (1, 2, 0, 3):
        z = 2 * p
        cells = jnp.concatenate([x[z + i : z + i + 2, j : j + 4].reshape(256, 128) for i, j in TAPS], axis=1)
        sums = jnp.dot(cells, weights, preferred_element_type=F32)
        out = jnp.maximum(three_taps(sums, 32, 128) + bias[...], 0.0)
        if p in (1, 2):
            skip[z - 2 : z] = out.astype(BF16).reshape(2, 4, 32, 128)
        most[...] = jnp.max(out.reshape(2, 2, 2, 32, 128), axis=(0, 2)).reshape(64, 128)
        small = jnp.maximum(most[pl.ds(0, 32, stride=2)], most[pl.ds(1, 32, stride=2)])
        pooled[p] = small.astype(BF16).reshape(2, 16, 128)


def level_b(shards, kernel, bias, skip, pooled, x, most):
    gz = lax.axis_index("gz")
    x[:, 0] = jnp.zeros((4, 16, 128), BF16)
    x[:, 9] = jnp.zeros((4, 16, 128), BF16)
    for g in range(4):
        x[:, 2 * g + 1 : 2 * g + 3] = shards[g]

    @pl.when(gz == 0)
    def _():
        x[0] = jnp.zeros((10, 16, 128), BF16)

    @pl.when(gz == lax.axis_size("gz") - 1)
    def _():
        x[3] = jnp.zeros((10, 16, 128), BF16)

    weights = jnp.concatenate(
        [jnp.concatenate([kernel[i, j, tap] for tap in range(3)], axis=0) for i, j in TAPS], axis=1
    )
    cells = jnp.concatenate([x[i : i + 2, j : j + 8].reshape(256, 128) for i, j in TAPS], axis=1)
    sums = lax.dot_general(cells, weights, (((1,), (1,)), ((), ())), preferred_element_type=F32)
    out = jnp.maximum(three_taps(sums, 16, 64) + bias[...], 0.0)
    skip[...] = out.astype(BF16).reshape(2, 8, 16, 64)
    most[...] = jnp.max(out.reshape(2, 4, 2, 16, 64), axis=(0, 2)).reshape(64, 64)
    small = jnp.maximum(most[pl.ds(0, 32, stride=2)], most[pl.ds(1, 32, stride=2)])
    pooled[...] = small.astype(BF16).reshape(1, 4, 8, 64)


def level_c(shards, kernel, bias, bottom, x):
    x[:, 0] = jnp.zeros((3, 8, 256), BF16)
    x[:, 5] = jnp.zeros((3, 8, 256), BF16)
    x[:, 1:5] = jnp.concatenate([shards[g] for g in range(4)], axis=-1)
    weights = jnp.concatenate(
        [jnp.concatenate([kernel[i, j, tap] for tap in range(3)], axis=1) for i, j in TAPS], axis=0
    )
    cells = jnp.concatenate([x[i, j : j + 4].reshape(32, 256) for i, j in TAPS], axis=1)
    sums = jnp.dot(cells, weights, preferred_element_type=F32)
    out = jnp.maximum(three_taps(sums, 8, 128) + bias[...], 0.0)
    bottom[...] = out.astype(BF16).reshape(1, 4, 8, 128)


def levels(volume, kernel_a, bias_a, kernel_b, bias_b, kernel_c, bias_c):
    pair, across = swap(*ends(volume, "gz", 3), "gz")
    wide, outward, inward = local(join, (volume, pair, across), [(10, 4, 32, 128), (10, 32, 128), (10, 32, 128)])
    pair, across = swap(outward, inward, "gy")
    skip_a, pooled_a = local(
        level_a,
        (wide, pair, across, kernel_a, bias_a[None]),
        [(4, 4, 32, 128), (4, 2, 16, 128)],
        [((10, 6, 32, 128), BF16), ((64, 128), F32)],
        1 << 30,
    )
    skip_b, pooled_b = local(
        level_b,
        (lax.all_gather(pooled_a, "gy"), jnp.swapaxes(kernel_b, 3, 4), bias_b[None]),
        [(2, 8, 16, 64), (1, 4, 8, 64)],
        [((4, 10, 16, 128), BF16), ((64, 64), F32)],
        1 << 28,
    )
    pair, across = swap(pooled_b, pooled_b, "gz")
    odd = lax.axis_index("gz") % 2
    partner = lax.dynamic_index_in_dim(pair, 1 - odd, 0, keepdims=False)
    deep = jnp.concatenate([jnp.where(odd == 1, partner, across), pooled_b, jnp.where(odd == 1, across, partner)])
    (bottom,) = local(
        level_c,
        (lax.all_gather(deep, "gy"), kernel_c, bias_c[None]),
        [(1, 4, 8, 128)],
        [((3, 6, 8, 256), BF16)],
        1 << 27,
    )
    return (skip_a, skip_b, bottom)


def solution(mesh):
    return jax.shard_map(
        levels,
        mesh=mesh,
        in_specs=(
            P("gz", "gy", None, None),
            P(),
            P(),
            P(None, None, None, None, "gy"),
            P("gy"),
            P(None, None, None, None, "gy"),
            P("gy"),
        ),
        out_specs=(P("gz", "gy", None, None), P("gz", None, None, "gy"), P("gz", None, None, "gy")),
        check_vma=False,
    )
```

```python
import jax
import jax.numpy as jnp
from jax import lax
from jax.experimental import pallas as pl
from jax.experimental.pallas import tpu as pltpu
from jax.sharding import PartitionSpec as P

BF16, F32 = jnp.bfloat16, jnp.float32


def even_groups(peers):
    return [[i, i + 1] for i in range(0, peers, 2)]


def odd_pairs(peers):
    pairs = [(i, i + 1) for i in range(1, peers - 1, 2)]
    return pairs + [(j, i) for i, j in pairs]


def swap(outward, inward, axis):
    peers = lax.axis_size(axis)
    across = lax.ppermute(outward, axis, odd_pairs(peers))
    pair = lax.all_gather(inward, axis, axis_index_groups=even_groups(peers))
    return pair, across


def local(body, inputs, outs, scratch=(), flops=0, kept=(), sems=0):
    vmem, kept_in_place = pl.BlockSpec(memory_space=pltpu.VMEM), pl.BlockSpec(memory_space=pltpu.HBM)
    specs = [kept_in_place if n in kept else vmem for n in range(len(inputs) + len(outs))]
    inputs = [pltpu.with_memory_space_constraint(a, pltpu.HBM) if n in kept else a for n, a in enumerate(inputs)]
    return pl.pallas_call(
        body,
        out_shape=[jax.ShapeDtypeStruct(*out) for out in outs],
        in_specs=specs[: len(inputs)],
        out_specs=specs[len(inputs) :],
        scratch_shapes=[pltpu.VMEM(*one) for one in scratch] + [pltpu.SemaphoreType.DMA((sems,))] * (sems > 0),
        cost_estimate=pl.CostEstimate(flops=flops, bytes_accessed=1 << 20, transcendentals=0),
        compiler_params=pltpu.CompilerParams(vmem_limit_bytes=32 << 20),
    )(*inputs)


def three_taps(wide, width, chans):
    cells = wide.shape[0]
    column = lax.broadcasted_iota(jnp.int32, (cells, chans), 0) % width
    left = jnp.where(column == 0, 0.0, pltpu.roll(wide[:, :chans], 1, 0))
    right = jnp.where(column == width - 1, 0.0, pltpu.roll(wide[:, 2 * chans :], cells - 1, 0))
    return left + wide[:, chans : 2 * chans] + right


TAPS = [(i, j) for i in range(3) for j in range(3)]


def edges(volume, own, outward, inward, sem):
    odd = lax.axis_index("gz") % 2
    read = pltpu.make_async_copy(volume, own, sem.at[0])
    read.start()
    read.wait()
    outward[...] = own[pl.ds(odd, 3)]
    inward[...] = own[pl.ds(1 - odd, 3)]


def fetch(kernel, bias, weights, offset, sem):
    reads = [pltpu.make_async_copy(bias, offset, sem.at[27])]
    for n, (i, j) in enumerate(TAPS):
        for tap in range(3):
            block = weights.at[128 * n : 128 * n + 128, 128 * tap : 128 * tap + 128]
            reads.append(pltpu.make_async_copy(kernel.at[i, j, tap], block, sem.at[3 * n + tap]))
    for read in reads:
        read.start()
    for read in reads:
        read.wait()


def join(volume, pair, across, wide, rows):
    odd, gy = lax.axis_index("gz") % 2, lax.axis_index("gy")
    wide[3:7] = volume[...]
    wide[pl.ds(7 * (1 - odd), 3)] = pair[1 - odd]
    wide[pl.ds(7 * odd, 3)] = across[...]
    rows[0] = wide[:, 3 * (1 - gy % 2)]
    rows[1] = wide[:, jnp.where(gy < 2, 2, 1)]


def level_a(wide, rows, weights, bias, skip, ship, x, most):
    gy = lax.axis_index("gy")
    core = gy % 2
    x[:, 1:5] = wide[...]
    x[:, 5 * (1 - core)] = rows[1 - core, 0]
    x[:, 5 * core] = jnp.zeros((10, 32, 128), BF16)
    open_row = jnp.where(gy == 1, 3, jnp.where(gy == 2, 0, 4))
    row = lax.broadcasted_iota(jnp.int32, (256, 128), 0) // 32 % 4
    for p in (1, 2, 0, 3):
        z = 2 * p
        cells = jnp.concatenate([x[z + i : z + i + 2, j : j + 4].reshape(256, 128) for i, j in TAPS], axis=1)
        sums = jnp.dot(cells, weights[...], preferred_element_type=F32)
        out = jnp.maximum(three_taps(sums, 32, 128) + bias[...], 0.0)
        if p in (1, 2):
            skip[z - 2 : z] = out.astype(BF16).reshape(2, 4, 32, 128)
        closed = jnp.where(row == open_row, 0.0, out)
        most[...] = jnp.max(closed.reshape(2, 2, 2, 32, 128), axis=(0, 2)).reshape(64, 128)
        small = jnp.maximum(most[pl.ds(0, 32, stride=2)], most[pl.ds(1, 32, stride=2)])
        ship[p] = small.astype(BF16)

    @pl.when((gy == 1) | (gy == 2))
    def _():
        ship[4:14] = wide[:, jnp.where(gy == 1, 3, 0)]

    @pl.when((gy == 0) | (gy == 3))
    def _():
        ship[4:14] = rows[1 - core, 1]


def level_b(ships, weights_a, bias_a, kernel, bias, patch, skip, pooled, x, most_a, most):
    gz, gy = lax.axis_index("gz"), lax.axis_index("gy")
    x[:, 0] = jnp.zeros((4, 16, 128), BF16)
    x[:, 9] = jnp.zeros((4, 16, 128), BF16)
    for g in range(4):
        x[:, 2 * g + 1 : 2 * g + 3] = ships[g, 0:4].reshape(4, 2, 16, 128)
    for r in range(2):
        cells = jnp.concatenate([ships[r + j, 4 + i : 12 + i].reshape(256, 128) for i, j in TAPS], axis=1)
        sums = jnp.dot(cells, weights_a[...], preferred_element_type=F32)
        out = jnp.maximum(three_taps(sums, 32, 128) + bias_a[...], 0.0)

        @pl.when(gy == r + 1)
        def _():
            patch[...] = out[64:192].astype(BF16).reshape(4, 32, 128)

        most_a[...] = jnp.max(out.reshape(4, 2, 32, 128), axis=1).reshape(128, 128)
        small = jnp.maximum(most_a[pl.ds(0, 64, stride=2)], most_a[pl.ds(1, 64, stride=2)])
        x[:, 4 + r] = jnp.maximum(x[:, 4 + r], small.astype(BF16).reshape(4, 16, 128))

    @pl.when(gz == 0)
    def _():
        x[0] = jnp.zeros((10, 16, 128), BF16)

    @pl.when(gz == lax.axis_size("gz") - 1)
    def _():
        x[3] = jnp.zeros((10, 16, 128), BF16)

    weights = jnp.concatenate(
        [jnp.concatenate([kernel[i, j, tap] for tap in range(3)], axis=0) for i, j in TAPS], axis=1
    )
    cells = jnp.concatenate([x[i : i + 2, j : j + 8].reshape(256, 128) for i, j in TAPS], axis=1)
    sums = lax.dot_general(cells, weights, (((1,), (1,)), ((), ())), preferred_element_type=F32)
    out = jnp.maximum(three_taps(sums, 16, 64) + bias[...], 0.0)
    skip[...] = out.astype(BF16).reshape(2, 8, 16, 64)
    most[...] = jnp.max(out.reshape(2, 4, 2, 16, 64), axis=(0, 2)).reshape(64, 64)
    small = jnp.maximum(most[pl.ds(0, 32, stride=2)], most[pl.ds(1, 32, stride=2)])
    pooled[...] = small.astype(BF16).reshape(1, 4, 8, 64)


def level_c(shards, kernel, bias, skip_a, patch, skip_b, bottom, out_a, out_b, x, whole, sem):
    gy = lax.axis_index("gy")
    write_b = pltpu.make_async_copy(skip_b, out_b, sem.at[1])
    write_b.start()
    whole[...] = skip_a[...]

    @pl.when(gy == 1)
    def _():
        whole[:, 3] = patch[...]

    @pl.when(gy == 2)
    def _():
        whole[:, 0] = patch[...]

    write_a = pltpu.make_async_copy(whole, out_a, sem.at[0])
    write_a.start()
    x[:, 0] = jnp.zeros((3, 8, 256), BF16)
    x[:, 5] = jnp.zeros((3, 8, 256), BF16)
    x[:, 1:5] = jnp.concatenate([shards[g] for g in range(4)], axis=-1)
    weights = jnp.concatenate(
        [jnp.concatenate([kernel[i, j, tap] for tap in range(3)], axis=1) for i, j in TAPS], axis=0
    )
    cells = jnp.concatenate([x[i, j : j + 4].reshape(32, 256) for i, j in TAPS], axis=1)
    sums = jnp.dot(cells, weights, preferred_element_type=F32)
    out = jnp.maximum(three_taps(sums, 8, 128) + bias[...], 0.0)
    bottom[...] = out.astype(BF16).reshape(1, 4, 8, 128)
    write_a.wait()
    write_b.wait()


def levels(volume, kernel_a, bias_a, kernel_b, bias_b, kernel_c, bias_c):
    slab = ((3, 4, 32, 128), BF16)
    own, outward, inward = local(edges, (volume,), [((4, 4, 32, 128), BF16), slab, slab], kept=(0,), sems=1)
    pair, across = swap(outward, inward, "gz")
    weights, offset = local(
        fetch, (kernel_a, bias_a[None]), [((1152, 384), BF16), ((1, 128), F32)], kept=(0, 1), sems=28
    )
    wide, rows = local(join, (own, pair, across), [((10, 4, 32, 128), BF16), ((2, 10, 32, 128), BF16)])
    rows = lax.all_gather(rows, "gy", axis_index_groups=even_groups(4))
    skip_a, ship = local(
        level_a,
        (wide, rows, weights, offset),
        [((4, 4, 32, 128), BF16), ((14, 32, 128), BF16)],
        [((10, 6, 32, 128), BF16), ((64, 128), F32)],
        1 << 30,
    )
    patch, skip_b, pooled_b = local(
        level_b,
        (lax.all_gather(ship, "gy"), weights, offset, jnp.swapaxes(kernel_b, 3, 4), bias_b[None]),
        [((4, 32, 128), BF16), ((2, 8, 16, 64), BF16), ((1, 4, 8, 64), BF16)],
        [((4, 10, 16, 128), BF16), ((128, 128), F32), ((64, 64), F32)],
        1 << 29,
    )
    pair, across = swap(pooled_b, pooled_b, "gz")
    odd = lax.axis_index("gz") % 2
    partner = lax.dynamic_index_in_dim(pair, 1 - odd, 0, keepdims=False)
    deep = jnp.concatenate([jnp.where(odd == 1, partner, across), pooled_b, jnp.where(odd == 1, across, partner)])
    bottom, skip_a, skip_b = local(
        level_c,
        (lax.all_gather(deep, "gy"), kernel_c, bias_c[None], skip_a, patch, skip_b),
        [((1, 4, 8, 128), BF16), ((4, 4, 32, 128), BF16), ((2, 8, 16, 64), BF16)],
        [((3, 6, 8, 256), BF16), ((4, 4, 32, 128), BF16)],
        1 << 27,
        kept=(7, 8),
        sems=2,
    )
    return (skip_a, skip_b, bottom)


def solution(mesh):
    return jax.shard_map(
        levels,
        mesh=mesh,
        in_specs=(
            P("gz", "gy", None, None),
            P(),
            P(),
            P(None, None, None, None, "gy"),
            P("gy"),
            P(None, None, None, None, "gy"),
            P("gy"),
        ),
        out_specs=(P("gz", "gy", None, None), P("gz", None, None, "gy"), P("gz", None, None, "gy")),
        check_vma=False,
    )
```

```python
import jax
import jax.numpy as jnp
from jax import lax
from jax.experimental import pallas as pl
from jax.experimental.pallas import tpu as pltpu
from jax.sharding import PartitionSpec as P

BF16, F32 = jnp.bfloat16, jnp.float32


def even_groups(peers):
    return [[i, i + 1] for i in range(0, peers, 2)]


def swap(outward, inward, axis):
    peers = lax.axis_size(axis)
    even = [(i, i ^ 1) for i in range(peers)]
    odd = [(i, i + 1) for i in range(1, peers - 1, 2)]
    across = lax.ppermute(outward, axis, odd + [(j, i) for i, j in odd])
    pair = lax.ppermute(inward, axis, even)
    return pair, across


def local(body, inputs, outs, scratch=(), flops=0, kept=(), sems=0, same={}):
    vmem, kept_in_place = pl.BlockSpec(memory_space=pltpu.VMEM), pl.BlockSpec(memory_space=pltpu.HBM)
    specs = [kept_in_place if n in kept else vmem for n in range(len(inputs) + len(outs))]
    inputs = [pltpu.with_memory_space_constraint(a, pltpu.HBM) if n in kept else a for n, a in enumerate(inputs)]
    return pl.pallas_call(
        body,
        out_shape=[jax.ShapeDtypeStruct(*out) for out in outs],
        in_specs=specs[: len(inputs)],
        out_specs=specs[len(inputs) :],
        input_output_aliases=same,
        scratch_shapes=[pltpu.VMEM(*one) for one in scratch] + [pltpu.SemaphoreType.DMA((sems,))] * (sems > 0),
        cost_estimate=pl.CostEstimate(flops=flops, bytes_accessed=1 << 20, transcendentals=0),
        compiler_params=pltpu.CompilerParams(vmem_limit_bytes=32 << 20),
    )(*inputs)


def three_taps(wide, width, chans):
    cells = wide.shape[0]
    column = lax.broadcasted_iota(jnp.int32, (cells, chans), 0) % width
    left = jnp.where(column == 0, 0.0, pltpu.roll(wide[:, :chans], 1, 0))
    right = jnp.where(column == width - 1, 0.0, pltpu.roll(wide[:, 2 * chans :], cells - 1, 0))
    return left + wide[:, chans : 2 * chans] + right


TAPS = [(i, j) for i in range(3) for j in range(3)]


def edges(volume, own, outward, inward, sem):
    odd = lax.axis_index("gz") % 2
    read = pltpu.make_async_copy(volume, own, sem.at[0])
    read.start()
    read.wait()
    outward[...] = own[pl.ds(odd, 3)]
    inward[...] = own[pl.ds(1 - odd, 3)]


def fetch(kernel, bias, weights, offset, sem):
    reads = [pltpu.make_async_copy(bias, offset, sem.at[27])]
    for n, (i, j) in enumerate(TAPS):
        for tap in range(3):
            block = weights.at[128 * n : 128 * n + 128, 128 * tap : 128 * tap + 128]
            reads.append(pltpu.make_async_copy(kernel.at[i, j, tap], block, sem.at[3 * n + tap]))
    for read in reads:
        read.start()
    for read in reads:
        read.wait()


def join(volume, pair, across, wide, rows):
    odd, gy = lax.axis_index("gz") % 2, lax.axis_index("gy")
    wide[3:7] = volume[...]
    wide[pl.ds(7 * (1 - odd), 3)] = pair[...]
    wide[pl.ds(7 * odd, 3)] = across[...]
    rows[0] = wide[:, 3 * (1 - gy % 2)]
    rows[1] = wide[:, jnp.where(gy < 2, 2, 1)]


def level_a(wide, rows, weights, bias, skip, ship, x, most, own, sem):
    gy = lax.axis_index("gy")
    core = gy % 2
    x[:, 1:5] = wide[...]
    x[:, 5 * (1 - core)] = rows[1 - core, 0]
    x[:, 5 * core] = jnp.zeros((10, 32, 128), BF16)
    open_row = jnp.where(gy == 1, 3, jnp.where(gy == 2, 0, 4))
    row = lax.broadcasted_iota(jnp.int32, (256, 128), 0) // 32 % 4
    for p in (1, 2, 0, 3):
        z = 2 * p
        cells = jnp.concatenate([x[z + i : z + i + 2, j : j + 4].reshape(256, 128) for i, j in TAPS], axis=1)
        sums = jnp.dot(cells, weights[...], preferred_element_type=F32)
        out = jnp.maximum(three_taps(sums, 32, 128) + bias[...], 0.0)
        if p in (1, 2):
            own[z - 2 : z] = out.astype(BF16).reshape(2, 4, 32, 128)
        if p == 2:
            write = pltpu.make_async_copy(own, skip, sem.at[0])
            write.start()
        closed = jnp.where(row == open_row, 0.0, out)
        most[...] = jnp.max(closed.reshape(2, 2, 2, 32, 128), axis=(0, 2)).reshape(64, 128)
        small = jnp.maximum(most[pl.ds(0, 32, stride=2)], most[pl.ds(1, 32, stride=2)])
        ship[p] = small.astype(BF16)

    @pl.when((gy == 1) | (gy == 2))
    def _():
        ship[4:14] = wide[:, jnp.where(gy == 1, 3, 0)]

    @pl.when((gy == 0) | (gy == 3))
    def _():
        ship[4:14] = rows[1 - core, 1]

    write.wait()


def level_b(ships, weights_a, bias_a, kernel, bias, patch, skip, pooled, x, most_a, most):
    gz, gy = lax.axis_index("gz"), lax.axis_index("gy")
    x[:, 0] = jnp.zeros((4, 16, 128), BF16)
    x[:, 9] = jnp.zeros((4, 16, 128), BF16)
    for g in range(4):
        x[:, 2 * g + 1 : 2 * g + 3] = ships[g, 0:4].reshape(4, 2, 16, 128)
    for r in range(2):
        cells = jnp.concatenate([ships[r + j, 4 + i : 12 + i].reshape(256, 128) for i, j in TAPS], axis=1)
        sums = jnp.dot(cells, weights_a[...], preferred_element_type=F32)
        out = jnp.maximum(three_taps(sums, 32, 128) + bias_a[...], 0.0)

        @pl.when(gy == r + 1)
        def _():
            patch[...] = out[64:192].astype(BF16).reshape(4, 32, 128)

        most_a[...] = jnp.max(out.reshape(4, 2, 32, 128), axis=1).reshape(128, 128)
        small = jnp.maximum(most_a[pl.ds(0, 64, stride=2)], most_a[pl.ds(1, 64, stride=2)])
        x[:, 4 + r] = jnp.maximum(x[:, 4 + r], small.astype(BF16).reshape(4, 16, 128))

    @pl.when(gz == 0)
    def _():
        x[0] = jnp.zeros((10, 16, 128), BF16)

    @pl.when(gz == lax.axis_size("gz") - 1)
    def _():
        x[3] = jnp.zeros((10, 16, 128), BF16)

    weights = jnp.concatenate(
        [jnp.concatenate([kernel[i, j, tap] for tap in range(3)], axis=0) for i, j in TAPS], axis=1
    )
    cells = jnp.concatenate([x[i : i + 2, j : j + 8].reshape(256, 128) for i, j in TAPS], axis=1)
    sums = lax.dot_general(cells, weights, (((1,), (1,)), ((), ())), preferred_element_type=F32)
    out = jnp.maximum(three_taps(sums, 16, 64) + bias[...], 0.0)
    skip[...] = out.astype(BF16).reshape(2, 8, 16, 64)
    most[...] = jnp.max(out.reshape(2, 4, 2, 16, 64), axis=(0, 2)).reshape(64, 64)
    small = jnp.maximum(most[pl.ds(0, 32, stride=2)], most[pl.ds(1, 32, stride=2)])
    pooled[...] = small.astype(BF16).reshape(1, 4, 8, 64)


def level_c(shards, kernel, bias, skip_a, patch, skip_b, bottom, out_a, out_b, x, sem):
    gy = lax.axis_index("gy")
    write_b = pltpu.make_async_copy(skip_b, out_b, sem.at[0])
    write_b.start()
    inner = (gy == 1) | (gy == 2)
    write_a = pltpu.make_async_copy(patch, out_a.at[:, jnp.where(gy == 1, 3, 0)], sem.at[1])

    @pl.when(inner)
    def _():
        write_a.start()

    x[:, 0] = jnp.zeros((3, 8, 256), BF16)
    x[:, 5] = jnp.zeros((3, 8, 256), BF16)
    x[:, 1:5] = jnp.concatenate([shards[g] for g in range(4)], axis=-1)
    weights = jnp.concatenate(
        [jnp.concatenate([kernel[i, j, tap] for tap in range(3)], axis=1) for i, j in TAPS], axis=0
    )
    cells = jnp.concatenate([x[i, j : j + 4].reshape(32, 256) for i, j in TAPS], axis=1)
    sums = jnp.dot(cells, weights, preferred_element_type=F32)
    out = jnp.maximum(three_taps(sums, 8, 128) + bias[...], 0.0)
    bottom[...] = out.astype(BF16).reshape(1, 4, 8, 128)
    write_b.wait()

    @pl.when(inner)
    def _():
        write_a.wait()


def levels(volume, kernel_a, bias_a, kernel_b, bias_b, kernel_c, bias_c):
    slab = ((3, 4, 32, 128), BF16)
    own, outward, inward = local(edges, (volume,), [((4, 4, 32, 128), BF16), slab, slab], kept=(0,), sems=1)
    pair, across = swap(outward, inward, "gz")
    weights, offset = local(
        fetch, (kernel_a, bias_a[None]), [((1152, 384), BF16), ((1, 128), F32)], kept=(0, 1), sems=28
    )
    wide, rows = local(join, (own, pair, across), [((10, 4, 32, 128), BF16), ((2, 10, 32, 128), BF16)])
    rows = lax.all_gather(rows, "gy", axis_index_groups=even_groups(4))
    skip_a, ship = local(
        level_a,
        (wide, rows, weights, offset),
        [((4, 4, 32, 128), BF16), ((14, 32, 128), BF16)],
        [((10, 6, 32, 128), BF16), ((64, 128), F32), ((4, 4, 32, 128), BF16)],
        1 << 30,
        kept=(4,),
        sems=1,
    )
    patch, skip_b, pooled_b = local(
        level_b,
        (lax.all_gather(ship, "gy"), weights, offset, jnp.swapaxes(kernel_b, 3, 4), bias_b[None]),
        [((4, 32, 128), BF16), ((2, 8, 16, 64), BF16), ((1, 4, 8, 64), BF16)],
        [((4, 10, 16, 128), BF16), ((128, 128), F32), ((64, 64), F32)],
        1 << 29,
    )
    pair, across = swap(pooled_b, pooled_b, "gz")
    odd = lax.axis_index("gz") % 2
    deep = jnp.concatenate([jnp.where(odd == 1, pair, across), pooled_b, jnp.where(odd == 1, across, pair)])
    bottom, skip_a, skip_b = local(
        level_c,
        (lax.all_gather(deep, "gy"), kernel_c, bias_c[None], skip_a, patch, skip_b),
        [((1, 4, 8, 128), BF16), ((4, 4, 32, 128), BF16), ((2, 8, 16, 64), BF16)],
        [((3, 6, 8, 256), BF16)],
        1 << 27,
        kept=(3, 7, 8),
        sems=2,
        same={3: 1},
    )
    return (skip_a, skip_b, bottom)


def solution(mesh):
    return jax.shard_map(
        levels,
        mesh=mesh,
        in_specs=(
            P("gz", "gy", None, None),
            P(),
            P(),
            P(None, None, None, None, "gy"),
            P("gy"),
            P(None, None, None, None, "gy"),
            P("gy"),
        ),
        out_specs=(P("gz", "gy", None, None), P("gz", None, None, "gy"), P("gz", None, None, "gy")),
        check_vma=False,
    )
```

```python
import jax
import jax.numpy as jnp
from jax import lax
from jax.experimental import pallas as pl
from jax.experimental.pallas import tpu as pltpu
from jax.sharding import PartitionSpec as P

BF16, F32 = jnp.bfloat16, jnp.float32


def even_groups(peers):
    return [[i, i + 1] for i in range(0, peers, 2)]


def odd_groups(peers, cores):
    inner = [[i * cores + c, (i + 1) * cores + c] for i in range(1, peers - 1, 2) for c in range(cores)]
    return inner + [[i * cores + c, i * cores + c + 1] for i in (0, peers - 1) for c in range(0, cores, 2)]


def swap(outward, inward):
    peers, cores = lax.axis_size("gz"), lax.axis_size("gy")
    pair = lax.ppermute(inward, "gz", [(i, i ^ 1) for i in range(peers)])
    across = lax.all_gather(outward, ("gz", "gy"), axis_index_groups=odd_groups(peers, cores))
    return pair, across


def at_end():
    gz = lax.axis_index("gz")
    return (gz == 0) | (gz == lax.axis_size("gz") - 1)


def local(body, inputs, outs, scratch=(), flops=0, kept=(), sems=0, same={}):
    vmem, kept_in_place = pl.BlockSpec(memory_space=pltpu.VMEM), pl.BlockSpec(memory_space=pltpu.HBM)
    specs = [kept_in_place if n in kept else vmem for n in range(len(inputs) + len(outs))]
    inputs = [pltpu.with_memory_space_constraint(a, pltpu.HBM) if n in kept else a for n, a in enumerate(inputs)]
    return pl.pallas_call(
        body,
        out_shape=[jax.ShapeDtypeStruct(*out) for out in outs],
        in_specs=specs[: len(inputs)],
        out_specs=specs[len(inputs) :],
        input_output_aliases=same,
        scratch_shapes=[pltpu.VMEM(*one) for one in scratch] + [pltpu.SemaphoreType.DMA((sems,))] * (sems > 0),
        cost_estimate=pl.CostEstimate(flops=flops, bytes_accessed=1 << 20, transcendentals=0),
        compiler_params=pltpu.CompilerParams(vmem_limit_bytes=32 << 20),
    )(*inputs)


def three_taps(wide, width, chans):
    cells = wide.shape[0]
    column = lax.broadcasted_iota(jnp.int32, (cells, chans), 0) % width
    left = jnp.where(column == 0, 0.0, pltpu.roll(wide[:, :chans], 1, 0))
    right = jnp.where(column == width - 1, 0.0, pltpu.roll(wide[:, 2 * chans :], cells - 1, 0))
    return left + wide[:, chans : 2 * chans] + right


TAPS = [(i, j) for i in range(3) for j in range(3)]


def edges(volume, kernel, bias, own, outward, inward, weights, offset, sem):
    odd = lax.axis_index("gz") % 2
    read = pltpu.make_async_copy(volume, own, sem.at[0])
    read.start()
    others = [pltpu.make_async_copy(kernel.at[i], weights.at[i], sem.at[i + 1]) for i in range(3)]
    others.append(pltpu.make_async_copy(bias, offset, sem.at[4]))
    for other in others:
        other.start()
    read.wait()
    outward[...] = own[pl.ds(odd, 3)]
    inward[...] = own[pl.ds(1 - odd, 3)]
    for other in others:
        other.wait()


def stacked(kernel, axis):
    taps = [jnp.concatenate([kernel[i, j, tap] for tap in range(3)], axis=axis) for i, j in TAPS]
    return jnp.concatenate(taps, axis=1 - axis)


def join(volume, pair, across, wide, rows):
    odd, gy = lax.axis_index("gz") % 2, lax.axis_index("gy")
    wide[3:7] = volume[...]
    wide[pl.ds(7 * (1 - odd), 3)] = pair[...]
    wide[pl.ds(7 * odd, 3)] = across[odd]

    @pl.when(at_end())
    def _():
        wide[pl.ds(7 * odd, 3)] = jnp.zeros((3, 4, 32, 128), BF16)

    rows[0] = wide[:, 3 * (1 - gy % 2)]
    rows[1] = wide[:, jnp.where(gy < 2, 2, 1)]


def level_a(wide, rows, kernel, bias, skip, ship, x, most):
    gy = lax.axis_index("gy")
    core = gy % 2
    x[:, 1:5] = wide[...]
    x[:, 5 * (1 - core)] = rows[1 - core, 0]
    x[:, 5 * core] = jnp.zeros((10, 32, 128), BF16)
    open_row = jnp.where(gy == 1, 3, jnp.where(gy == 2, 0, 4))
    row = lax.broadcasted_iota(jnp.int32, (256, 128), 0) // 32 % 4
    weights = stacked(kernel, 1)
    for p in (1, 2, 0, 3):
        z = 2 * p
        cells = jnp.concatenate([x[z + i : z + i + 2, j : j + 4].reshape(256, 128) for i, j in TAPS], axis=1)
        sums = jnp.dot(cells, weights, preferred_element_type=F32)
        out = jnp.maximum(three_taps(sums, 32, 128) + bias[...], 0.0)
        if p in (1, 2):
            skip[z - 2 : z] = out.astype(BF16).reshape(2, 4, 32, 128)
        closed = jnp.where(row == open_row, 0.0, out)
        most[...] = jnp.max(closed.reshape(2, 2, 2, 32, 128), axis=(0, 2)).reshape(64, 128)
        small = jnp.maximum(most[pl.ds(0, 32, stride=2)], most[pl.ds(1, 32, stride=2)])
        ship[p] = small.astype(BF16)

    @pl.when((gy == 1) | (gy == 2))
    def _():
        ship[4:14] = wide[:, jnp.where(gy == 1, 3, 0)]

    @pl.when((gy == 0) | (gy == 3))
    def _():
        ship[4:14] = rows[1 - core, 1]


def level_b(ships, kernel_a, bias_a, kernel, bias, skip_a, patch, skip, pooled, out_a, x, most_a, most, sem):
    gz, gy = lax.axis_index("gz"), lax.axis_index("gy")
    write = pltpu.make_async_copy(skip_a, out_a, sem.at[0])
    write.start()
    weights_a = stacked(kernel_a, 1)
    x[:, 0] = jnp.zeros((4, 16, 128), BF16)
    x[:, 9] = jnp.zeros((4, 16, 128), BF16)
    for g in range(4):
        x[:, 2 * g + 1 : 2 * g + 3] = ships[g, 0:4].reshape(4, 2, 16, 128)
    for r in range(2):
        cells = jnp.concatenate([ships[r + j, 4 + i : 12 + i].reshape(256, 128) for i, j in TAPS], axis=1)
        sums = jnp.dot(cells, weights_a, preferred_element_type=F32)
        out = jnp.maximum(three_taps(sums, 32, 128) + bias_a[...], 0.0)

        @pl.when(gy == r + 1)
        def _():
            patch[...] = out[64:192].astype(BF16).reshape(4, 32, 128)

        most_a[...] = jnp.max(out.reshape(4, 2, 32, 128), axis=1).reshape(128, 128)
        small = jnp.maximum(most_a[pl.ds(0, 64, stride=2)], most_a[pl.ds(1, 64, stride=2)])
        x[:, 4 + r] = jnp.maximum(x[:, 4 + r], small.astype(BF16).reshape(4, 16, 128))

    @pl.when(gz == 0)
    def _():
        x[0] = jnp.zeros((10, 16, 128), BF16)

    @pl.when(gz == lax.axis_size("gz") - 1)
    def _():
        x[3] = jnp.zeros((10, 16, 128), BF16)

    weights = stacked(kernel, 0)
    cells = jnp.concatenate([x[i : i + 2, j : j + 8].reshape(256, 128) for i, j in TAPS], axis=1)
    sums = lax.dot_general(cells, weights, (((1,), (1,)), ((), ())), preferred_element_type=F32)
    out = jnp.maximum(three_taps(sums, 16, 64) + bias[...], 0.0)
    skip[...] = out.astype(BF16).reshape(2, 8, 16, 64)
    most[...] = jnp.max(out.reshape(2, 4, 2, 16, 64), axis=(0, 2)).reshape(64, 64)
    small = jnp.maximum(most[pl.ds(0, 32, stride=2)], most[pl.ds(1, 32, stride=2)])
    pooled[...] = small.astype(BF16).reshape(1, 4, 8, 64)
    write.wait()


def level_c(shards, kernel, bias, skip_a, patch, skip_b, bottom, out_a, out_b, x, sem):
    gy = lax.axis_index("gy")
    write_b = pltpu.make_async_copy(skip_b, out_b, sem.at[0])
    write_b.start()
    inner = (gy == 1) | (gy == 2)
    write_a = pltpu.make_async_copy(patch, out_a.at[:, jnp.where(gy == 1, 3, 0)], sem.at[1])

    @pl.when(inner)
    def _():
        write_a.start()

    x[:, 0] = jnp.zeros((3, 8, 256), BF16)
    x[:, 5] = jnp.zeros((3, 8, 256), BF16)
    x[:, 1:5] = jnp.concatenate([shards[g] for g in range(4)], axis=-1)
    weights = stacked(kernel, 1)
    cells = jnp.concatenate([x[i, j : j + 4].reshape(32, 256) for i, j in TAPS], axis=1)
    sums = jnp.dot(cells, weights, preferred_element_type=F32)
    out = jnp.maximum(three_taps(sums, 8, 128) + bias[...], 0.0)
    bottom[...] = out.astype(BF16).reshape(1, 4, 8, 128)
    write_b.wait()

    @pl.when(inner)
    def _():
        write_a.wait()


def levels(volume, kernel_a, bias_a, kernel_b, bias_b, kernel_c, bias_c):
    slab = ((3, 4, 32, 128), BF16)
    own, outward, inward, weights, offset = local(
        edges,
        (volume, kernel_a, bias_a[None]),
        [((4, 4, 32, 128), BF16), slab, slab, (kernel_a.shape, BF16), ((1, 128), F32)],
        kept=(0, 1, 2),
        sems=5,
    )
    pair, across = swap(outward, inward)
    wide, rows = local(join, (own, pair, across), [((10, 4, 32, 128), BF16), ((2, 10, 32, 128), BF16)])
    rows = lax.all_gather(rows, "gy", axis_index_groups=even_groups(4))
    skip_a, ship = local(
        level_a,
        (wide, rows, weights, offset),
        [((4, 4, 32, 128), BF16), ((14, 32, 128), BF16)],
        [((10, 6, 32, 128), BF16), ((64, 128), F32)],
        1 << 30,
    )
    patch, skip_b, pooled_b, skip_a = local(
        level_b,
        (lax.all_gather(ship, "gy"), weights, offset, jnp.swapaxes(kernel_b, 3, 4), bias_b[None], skip_a),
        [((4, 32, 128), BF16), ((2, 8, 16, 64), BF16), ((1, 4, 8, 64), BF16), ((4, 4, 32, 128), BF16)],
        [((4, 10, 16, 128), BF16), ((128, 128), F32), ((64, 64), F32)],
        1 << 29,
        kept=(9,),
        sems=1,
    )
    pair, across = swap(pooled_b, pooled_b)
    odd = lax.axis_index("gz") % 2
    across = jnp.where(at_end(), BF16(0), lax.dynamic_index_in_dim(across, odd, 0, keepdims=False))
    deep = jnp.concatenate([jnp.where(odd == 1, pair, across), pooled_b, jnp.where(odd == 1, across, pair)])
    bottom, skip_a, skip_b = local(
        level_c,
        (lax.all_gather(deep, "gy"), kernel_c, bias_c[None], skip_a, patch, skip_b),
        [((1, 4, 8, 128), BF16), ((4, 4, 32, 128), BF16), ((2, 8, 16, 64), BF16)],
        [((3, 6, 8, 256), BF16)],
        1 << 27,
        kept=(3, 7, 8),
        sems=2,
        same={3: 1},
    )
    return (skip_a, skip_b, bottom)


def solution(mesh):
    return jax.shard_map(
        levels,
        mesh=mesh,
        in_specs=(
            P("gz", "gy", None, None),
            P(),
            P(),
            P(None, None, None, None, "gy"),
            P("gy"),
            P(None, None, None, None, "gy"),
            P("gy"),
        ),
        out_specs=(P("gz", "gy", None, None), P("gz", None, None, "gy"), P("gz", None, None, "gy")),
        check_vma=False,
    )
```

```python
import jax
import jax.numpy as jnp
from jax import lax
from jax.experimental import pallas as pl
from jax.experimental.pallas import tpu as pltpu
from jax.sharding import PartitionSpec as P

BF16, F32 = jnp.bfloat16, jnp.float32


def even_groups(peers):
    return [[i, i + 1] for i in range(0, peers, 2)]


def swap(outward, inward):
    peers = lax.axis_size("gz")
    odd = [(i, i + 1) for i in range(1, peers - 1, 2)]
    pair = lax.ppermute(inward, "gz", [(i, i ^ 1) for i in range(peers)])
    across = lax.ppermute(outward, "gz", odd + [(j, i) for i, j in odd])
    return pair, across


def local(body, inputs, outs, scratch=(), flops=0, kept=(), sems=0, same={}):
    vmem, kept_in_place = pl.BlockSpec(memory_space=pltpu.VMEM), pl.BlockSpec(memory_space=pltpu.HBM)
    specs = [kept_in_place if n in kept else vmem for n in range(len(inputs) + len(outs))]
    inputs = [pltpu.with_memory_space_constraint(a, pltpu.HBM) if n in kept else a for n, a in enumerate(inputs)]
    return pl.pallas_call(
        body,
        out_shape=[jax.ShapeDtypeStruct(*out) for out in outs],
        in_specs=specs[: len(inputs)],
        out_specs=specs[len(inputs) :],
        input_output_aliases=same,
        scratch_shapes=[pltpu.VMEM(*one) for one in scratch] + [pltpu.SemaphoreType.DMA((sems,))] * (sems > 0),
        cost_estimate=pl.CostEstimate(flops=flops, bytes_accessed=1 << 20, transcendentals=0),
        compiler_params=pltpu.CompilerParams(vmem_limit_bytes=32 << 20),
    )(*inputs)


def three_taps(wide, width, chans):
    cells = wide.shape[0]
    column = lax.broadcasted_iota(jnp.int32, (cells, chans), 0) % width
    left = jnp.where(column == 0, 0.0, pltpu.roll(wide[:, :chans], 1, 0))
    right = jnp.where(column == width - 1, 0.0, pltpu.roll(wide[:, 2 * chans :], cells - 1, 0))
    return left + wide[:, chans : 2 * chans] + right


TAPS = [(i, j) for i in range(3) for j in range(3)]


def edges(volume, kernel, bias, own, outward, inward, weights, offset, sem):
    odd = lax.axis_index("gz") % 2
    read = pltpu.make_async_copy(volume, own, sem.at[0])
    read.start()
    others = [pltpu.make_async_copy(kernel.at[i], weights.at[i], sem.at[i + 1]) for i in range(3)]
    others.append(pltpu.make_async_copy(bias, offset, sem.at[4]))
    for other in others:
        other.start()
    read.wait()
    outward[...] = own[pl.ds(odd, 3)]
    inward[...] = own[pl.ds(1 - odd, 3)]
    for other in others:
        other.wait()


def stacked(kernel, axis):
    taps = [jnp.concatenate([kernel[i, j, tap] for tap in range(3)], axis=axis) for i, j in TAPS]
    return jnp.concatenate(taps, axis=1 - axis)


def join(volume, pair, across, wide, rows):
    odd, gy = lax.axis_index("gz") % 2, lax.axis_index("gy")
    wide[3:7] = volume[...]
    wide[pl.ds(7 * (1 - odd), 3)] = pair[...]
    wide[pl.ds(7 * odd, 3)] = across[...]
    rows[0] = wide[:, 3 * (1 - gy % 2)]
    rows[1] = wide[:, jnp.where(gy < 2, 2, 1)]


def level_a(wide, rows, kernel, bias, skip, ship, x, most):
    gy = lax.axis_index("gy")
    core = gy % 2
    x[:, 1:5] = wide[...]
    x[:, 5 * (1 - core)] = rows[1 - core, 0]
    x[:, 5 * core] = jnp.zeros((10, 32, 128), BF16)
    open_row = jnp.where(gy == 1, 3, jnp.where(gy == 2, 0, 4))
    row = lax.broadcasted_iota(jnp.int32, (256, 128), 0) // 32 % 4
    weights = stacked(kernel, 1)
    for p in (1, 2, 0, 3):
        z = 2 * p
        cells = jnp.concatenate([x[z + i : z + i + 2, j : j + 4].reshape(256, 128) for i, j in TAPS], axis=1)
        sums = jnp.dot(cells, weights, preferred_element_type=F32)
        out = jnp.maximum(three_taps(sums, 32, 128) + bias[...], 0.0)
        if p in (1, 2):
            skip[z - 2 : z] = out.astype(BF16).reshape(2, 4, 32, 128)
        closed = jnp.where(row == open_row, 0.0, out)
        most[...] = jnp.max(closed.reshape(2, 2, 2, 32, 128), axis=(0, 2)).reshape(64, 128)
        small = jnp.maximum(most[pl.ds(0, 32, stride=2)], most[pl.ds(1, 32, stride=2)])
        ship[p] = small.astype(BF16)

    @pl.when((gy == 1) | (gy == 2))
    def _():
        ship[4:14] = wide[:, jnp.where(gy == 1, 3, 0)]

    @pl.when((gy == 0) | (gy == 3))
    def _():
        ship[4:14] = rows[1 - core, 1]


def level_b(ships, kernel_a, bias_a, kernel, bias, skip_a, patch, skip, pooled, out_a, x, most_a, most, sem):
    gz, gy = lax.axis_index("gz"), lax.axis_index("gy")
    write = pltpu.make_async_copy(skip_a, out_a, sem.at[0])
    write.start()
    weights_a = stacked(kernel_a, 1)
    x[:, 0] = jnp.zeros((4, 16, 128), BF16)
    x[:, 9] = jnp.zeros((4, 16, 128), BF16)
    for g in range(4):
        x[:, 2 * g + 1 : 2 * g + 3] = ships[g, 0:4].reshape(4, 2, 16, 128)
    for r in range(2):
        cells = jnp.concatenate([ships[r + j, 4 + i : 12 + i].reshape(256, 128) for i, j in TAPS], axis=1)
        sums = jnp.dot(cells, weights_a, preferred_element_type=F32)
        out = jnp.maximum(three_taps(sums, 32, 128) + bias_a[...], 0.0)

        @pl.when(gy == r + 1)
        def _():
            patch[...] = out[64:192].astype(BF16).reshape(4, 32, 128)

        most_a[...] = jnp.max(out.reshape(4, 2, 32, 128), axis=1).reshape(128, 128)
        small = jnp.maximum(most_a[pl.ds(0, 64, stride=2)], most_a[pl.ds(1, 64, stride=2)])
        x[:, 4 + r] = jnp.maximum(x[:, 4 + r], small.astype(BF16).reshape(4, 16, 128))

    @pl.when(gz == 0)
    def _():
        x[0] = jnp.zeros((10, 16, 128), BF16)

    @pl.when(gz == lax.axis_size("gz") - 1)
    def _():
        x[3] = jnp.zeros((10, 16, 128), BF16)

    weights = stacked(kernel, 0)
    cells = jnp.concatenate([x[i : i + 2, j : j + 8].reshape(256, 128) for i, j in TAPS], axis=1)
    sums = lax.dot_general(cells, weights, (((1,), (1,)), ((), ())), preferred_element_type=F32)
    out = jnp.maximum(three_taps(sums, 16, 64) + bias[...], 0.0)
    skip[...] = out.astype(BF16).reshape(2, 8, 16, 64)
    most[...] = jnp.max(out.reshape(2, 4, 2, 16, 64), axis=(0, 2)).reshape(64, 64)
    small = jnp.maximum(most[pl.ds(0, 32, stride=2)], most[pl.ds(1, 32, stride=2)])
    pooled[...] = small.astype(BF16).reshape(1, 4, 8, 64)
    write.wait()


def level_c(shards, kernel, bias, skip_a, patch, skip_b, bottom, out_a, out_b, x, sem):
    gy = lax.axis_index("gy")
    write_b = pltpu.make_async_copy(skip_b, out_b, sem.at[0])
    write_b.start()
    inner = (gy == 1) | (gy == 2)
    write_a = pltpu.make_async_copy(patch, out_a.at[:, jnp.where(gy == 1, 3, 0)], sem.at[1])

    @pl.when(inner)
    def _():
        write_a.start()

    x[:, 0] = jnp.zeros((3, 8, 256), BF16)
    x[:, 5] = jnp.zeros((3, 8, 256), BF16)
    x[:, 1:5] = jnp.concatenate([shards[g] for g in range(4)], axis=-1)
    weights = stacked(kernel, 1)
    cells = jnp.concatenate([x[i, j : j + 4].reshape(32, 256) for i, j in TAPS], axis=1)
    sums = jnp.dot(cells, weights, preferred_element_type=F32)
    out = jnp.maximum(three_taps(sums, 8, 128) + bias[...], 0.0)
    bottom[...] = out.astype(BF16).reshape(1, 4, 8, 128)
    write_b.wait()

    @pl.when(inner)
    def _():
        write_a.wait()


def levels(volume, kernel_a, bias_a, kernel_b, bias_b, kernel_c, bias_c):
    slab = ((3, 4, 32, 128), BF16)
    own, outward, inward, weights, offset = local(
        edges,
        (volume, kernel_a, bias_a[None]),
        [((4, 4, 32, 128), BF16), slab, slab, (kernel_a.shape, BF16), ((1, 128), F32)],
        kept=(0, 1, 2),
        sems=5,
    )
    pair, across = swap(outward, inward)
    wide, rows = local(join, (own, pair, across), [((10, 4, 32, 128), BF16), ((2, 10, 32, 128), BF16)])
    rows = lax.all_gather(rows, "gy", axis_index_groups=even_groups(4))
    skip_a, ship = local(
        level_a,
        (wide, rows, weights, offset),
        [((4, 4, 32, 128), BF16), ((14, 32, 128), BF16)],
        [((10, 6, 32, 128), BF16), ((64, 128), F32)],
        1 << 30,
    )
    patch, skip_b, pooled_b, skip_a = local(
        level_b,
        (lax.all_gather(ship, "gy"), weights, offset, jnp.swapaxes(kernel_b, 3, 4), bias_b[None], skip_a),
        [((4, 32, 128), BF16), ((2, 8, 16, 64), BF16), ((1, 4, 8, 64), BF16), ((4, 4, 32, 128), BF16)],
        [((4, 10, 16, 128), BF16), ((128, 128), F32), ((64, 64), F32)],
        1 << 29,
        kept=(9,),
        sems=1,
    )
    pair, across = swap(pooled_b, pooled_b)
    odd = lax.axis_index("gz") % 2
    deep = jnp.concatenate([jnp.where(odd == 1, pair, across), pooled_b, jnp.where(odd == 1, across, pair)])
    bottom, skip_a, skip_b = local(
        level_c,
        (lax.all_gather(deep, "gy"), kernel_c, bias_c[None], skip_a, patch, skip_b),
        [((1, 4, 8, 128), BF16), ((4, 4, 32, 128), BF16), ((2, 8, 16, 64), BF16)],
        [((3, 6, 8, 256), BF16)],
        1 << 27,
        kept=(3, 7, 8),
        sems=2,
        same={3: 1},
    )
    return (skip_a, skip_b, bottom)


def solution(mesh):
    return jax.shard_map(
        levels,
        mesh=mesh,
        in_specs=(
            P("gz", "gy", None, None),
            P(),
            P(),
            P(None, None, None, None, "gy"),
            P("gy"),
            P(None, None, None, None, "gy"),
            P("gy"),
        ),
        out_specs=(P("gz", "gy", None, None), P("gz", None, None, "gy"), P("gz", None, None, "gy")),
        check_vma=False,
    )
```

```python
import jax
import jax.numpy as jnp
from jax import lax
from jax.experimental import pallas as pl
from jax.experimental.pallas import tpu as pltpu
from jax.sharding import PartitionSpec as P

BF16, F32 = jnp.bfloat16, jnp.float32


def even_groups(peers):
    return [[i, i + 1] for i in range(0, peers, 2)]


def odd_groups(peers, cores):
    inner = [[i * cores + c, (i + 1) * cores + c] for i in range(1, peers - 1, 2) for c in range(cores)]
    return inner + [[i * cores + c, i * cores + c + 1] for i in (0, peers - 1) for c in range(0, cores, 2)]


def swap(outward, inward):
    peers, cores = lax.axis_size("gz"), lax.axis_size("gy")
    pair = lax.ppermute(inward, "gz", [(i, i ^ 1) for i in range(peers)])
    across = lax.all_gather(outward, ("gz", "gy"), axis_index_groups=odd_groups(peers, cores))
    return pair, across


def at_end():
    gz = lax.axis_index("gz")
    return (gz == 0) | (gz == lax.axis_size("gz") - 1)


def local(body, inputs, outs, scratch=(), flops=0, kept=(), sems=0, same={}):
    vmem, kept_in_place = pl.BlockSpec(memory_space=pltpu.VMEM), pl.BlockSpec(memory_space=pltpu.HBM)
    specs = [kept_in_place if n in kept else vmem for n in range(len(inputs) + len(outs))]
    inputs = [pltpu.with_memory_space_constraint(a, pltpu.HBM) if n in kept else a for n, a in enumerate(inputs)]
    return pl.pallas_call(
        body,
        out_shape=[jax.ShapeDtypeStruct(*out) for out in outs],
        in_specs=specs[: len(inputs)],
        out_specs=specs[len(inputs) :],
        input_output_aliases=same,
        scratch_shapes=[pltpu.VMEM(*one) for one in scratch] + [pltpu.SemaphoreType.DMA((sems,))] * (sems > 0),
        cost_estimate=pl.CostEstimate(flops=flops, bytes_accessed=1 << 20, transcendentals=0),
        compiler_params=pltpu.CompilerParams(vmem_limit_bytes=32 << 20),
    )(*inputs)


def three_taps(wide, width, chans):
    cells = wide.shape[0]
    column = lax.broadcasted_iota(jnp.int32, (cells, chans), 0) % width
    left = jnp.where(column == 0, 0.0, pltpu.roll(wide[:, :chans], 1, 0))
    right = jnp.where(column == width - 1, 0.0, pltpu.roll(wide[:, 2 * chans :], cells - 1, 0))
    return left + wide[:, chans : 2 * chans] + right


TAPS = [(i, j) for i in range(3) for j in range(3)]


def edges(volume, own, outward, inward, sem):
    odd = lax.axis_index("gz") % 2
    read = pltpu.make_async_copy(volume, own, sem.at[0])
    read.start()
    read.wait()
    outward[...] = own[pl.ds(odd, 3)]
    inward[...] = own[pl.ds(1 - odd, 3)]


def stacked(kernel, axis):
    taps = [jnp.concatenate([kernel[i, j, tap] for tap in range(3)], axis=axis) for i, j in TAPS]
    return jnp.concatenate(taps, axis=1 - axis)


def join(volume, pair, across, wide, rows):
    odd, gy = lax.axis_index("gz") % 2, lax.axis_index("gy")
    wide[3:7] = volume[...]
    wide[pl.ds(7 * (1 - odd), 3)] = pair[...]
    wide[pl.ds(7 * odd, 3)] = across[odd]

    @pl.when(at_end())
    def _():
        wide[pl.ds(7 * odd, 3)] = jnp.zeros((3, 4, 32, 128), BF16)

    rows[0] = wide[:, 3 * (1 - gy % 2)]
    rows[1] = wide[:, jnp.where(gy < 2, 2, 1)]


def level_a(wide, rows, kernel, bias, skip, ship, x, most):
    gy = lax.axis_index("gy")
    core = gy % 2
    x[:, 1:5] = wide[...]
    x[:, 5 * (1 - core)] = rows[1 - core, 0]
    x[:, 5 * core] = jnp.zeros((10, 32, 128), BF16)
    open_row = jnp.where(gy == 1, 3, jnp.where(gy == 2, 0, 4))
    row = lax.broadcasted_iota(jnp.int32, (256, 128), 0) // 32 % 4
    weights = stacked(kernel, 1)
    for p in (1, 2, 0, 3):
        z = 2 * p
        cells = jnp.concatenate([x[z + i : z + i + 2, j : j + 4].reshape(256, 128) for i, j in TAPS], axis=1)
        sums = jnp.dot(cells, weights, preferred_element_type=F32)
        out = jnp.maximum(three_taps(sums, 32, 128) + bias[...], 0.0)
        if p in (1, 2):
            skip[z - 2 : z] = out.astype(BF16).reshape(2, 4, 32, 128)
        closed = jnp.where(row == open_row, 0.0, out)
        most[...] = jnp.max(closed.reshape(2, 2, 2, 32, 128), axis=(0, 2)).reshape(64, 128)
        small = jnp.maximum(most[pl.ds(0, 32, stride=2)], most[pl.ds(1, 32, stride=2)])
        ship[p] = small.astype(BF16)

    @pl.when((gy == 1) | (gy == 2))
    def _():
        ship[4:14] = wide[:, jnp.where(gy == 1, 3, 0)]

    @pl.when((gy == 0) | (gy == 3))
    def _():
        ship[4:14] = rows[1 - core, 1]


def level_b(ships, kernel_a, bias_a, kernel, bias, skip_a, patch, skip, pooled, out_a, x, most_a, most, sem):
    gz, gy = lax.axis_index("gz"), lax.axis_index("gy")
    write = pltpu.make_async_copy(skip_a, out_a, sem.at[0])
    write.start()
    weights_a = stacked(kernel_a, 1)
    x[:, 0] = jnp.zeros((4, 16, 128), BF16)
    x[:, 9] = jnp.zeros((4, 16, 128), BF16)
    for g in range(4):
        x[:, 2 * g + 1 : 2 * g + 3] = ships[g, 0:4].reshape(4, 2, 16, 128)
    for r in range(2):
        cells = jnp.concatenate([ships[r + j, 4 + i : 12 + i].reshape(256, 128) for i, j in TAPS], axis=1)
        sums = jnp.dot(cells, weights_a, preferred_element_type=F32)
        out = jnp.maximum(three_taps(sums, 32, 128) + bias_a[...], 0.0)

        @pl.when(gy == r + 1)
        def _():
            patch[...] = out[64:192].astype(BF16).reshape(4, 32, 128)

        most_a[...] = jnp.max(out.reshape(4, 2, 32, 128), axis=1).reshape(128, 128)
        small = jnp.maximum(most_a[pl.ds(0, 64, stride=2)], most_a[pl.ds(1, 64, stride=2)])
        x[:, 4 + r] = jnp.maximum(x[:, 4 + r], small.astype(BF16).reshape(4, 16, 128))

    @pl.when(gz == 0)
    def _():
        x[0] = jnp.zeros((10, 16, 128), BF16)

    @pl.when(gz == lax.axis_size("gz") - 1)
    def _():
        x[3] = jnp.zeros((10, 16, 128), BF16)

    weights = stacked(kernel, 0)
    cells = jnp.concatenate([x[i : i + 2, j : j + 8].reshape(256, 128) for i, j in TAPS], axis=1)
    sums = lax.dot_general(cells, weights, (((1,), (1,)), ((), ())), preferred_element_type=F32)
    out = jnp.maximum(three_taps(sums, 16, 64) + bias[...], 0.0)
    skip[...] = out.astype(BF16).reshape(2, 8, 16, 64)
    most[...] = jnp.max(out.reshape(2, 4, 2, 16, 64), axis=(0, 2)).reshape(64, 64)
    small = jnp.maximum(most[pl.ds(0, 32, stride=2)], most[pl.ds(1, 32, stride=2)])
    pooled[...] = small.astype(BF16).reshape(1, 4, 8, 64)
    write.wait()


def level_c(own, pair, across, kernel, bias, skip_a, patch, skip_b, bottom, out_a, out_b, x, sem):
    gy = lax.axis_index("gy")
    write_b = pltpu.make_async_copy(skip_b, out_b, sem.at[0])
    write_b.start()
    inner = (gy == 1) | (gy == 2)
    write_a = pltpu.make_async_copy(patch, out_a.at[:, jnp.where(gy == 1, 3, 0)], sem.at[1])

    @pl.when(inner)
    def _():
        write_a.start()

    x[:, 0] = jnp.zeros((3, 8, 256), BF16)
    x[:, 5] = jnp.zeros((3, 8, 256), BF16)
    odd = lax.axis_index("gz") % 2
    x[1, 1:5] = jnp.concatenate([own[g] for g in range(4)], axis=-1)
    x[2 * (1 - odd), 1:5] = jnp.concatenate([pair[g] for g in range(4)], axis=-1)
    x[2 * odd, 1:5] = jnp.concatenate([across[odd, g] for g in range(4)], axis=-1)

    @pl.when(at_end())
    def _():
        x[2 * odd, 1:5] = jnp.zeros((4, 8, 256), BF16)

    weights = stacked(kernel, 1)
    cells = jnp.concatenate([x[i, j : j + 4].reshape(32, 256) for i, j in TAPS], axis=1)
    sums = jnp.dot(cells, weights, preferred_element_type=F32)
    out = jnp.maximum(three_taps(sums, 8, 128) + bias[...], 0.0)
    bottom[...] = out.astype(BF16).reshape(1, 4, 8, 128)
    write_b.wait()

    @pl.when(inner)
    def _():
        write_a.wait()


def levels(volume, kernel_a, bias_a, kernel_b, bias_b, kernel_c, bias_c):
    slab = ((3, 4, 32, 128), BF16)
    own, outward, inward = local(edges, (volume,), [((4, 4, 32, 128), BF16), slab, slab], kept=(0,), sems=1)
    pair, across = swap(outward, inward)
    joined = [((10, 4, 32, 128), BF16), ((2, 10, 32, 128), BF16)]
    wide, rows = local(join, (own, pair, across), joined, flops=1 << 33)
    rows = lax.all_gather(rows, "gy", axis_index_groups=even_groups(4))
    skip_a, ship = local(
        level_a,
        (wide, rows, kernel_a, bias_a[None]),
        [((4, 4, 32, 128), BF16), ((14, 32, 128), BF16)],
        [((10, 6, 32, 128), BF16), ((64, 128), F32)],
        1 << 30,
    )
    patch, skip_b, pooled_b, skip_a = local(
        level_b,
        (lax.all_gather(ship, "gy"), kernel_a, bias_a[None], jnp.swapaxes(kernel_b, 3, 4), bias_b[None], skip_a),
        [((4, 32, 128), BF16), ((2, 8, 16, 64), BF16), ((1, 4, 8, 64), BF16), ((4, 4, 32, 128), BF16)],
        [((4, 10, 16, 128), BF16), ((128, 128), F32), ((64, 64), F32)],
        1 << 29,
        kept=(9,),
        sems=1,
    )
    channels = lax.all_gather(pooled_b, "gy", tiled=True)
    pair, across = swap(channels, channels)
    bottom, skip_a, skip_b = local(
        level_c,
        (channels, pair, across, kernel_c, bias_c[None], skip_a, patch, skip_b),
        [((1, 4, 8, 128), BF16), ((4, 4, 32, 128), BF16), ((2, 8, 16, 64), BF16)],
        [((3, 6, 8, 256), BF16)],
        1 << 27,
        kept=(5, 9, 10),
        sems=2,
        same={5: 1},
    )
    return (skip_a, skip_b, bottom)


def solution(mesh):
    return jax.shard_map(
        levels,
        mesh=mesh,
        in_specs=(
            P("gz", "gy", None, None),
            P(),
            P(),
            P(None, None, None, None, "gy"),
            P("gy"),
            P(None, None, None, None, "gy"),
            P("gy"),
        ),
        out_specs=(P("gz", "gy", None, None), P("gz", None, None, "gy"), P("gz", None, None, "gy")),
        check_vma=False,
    )
```

```python
import jax
import jax.numpy as jnp
from jax import lax
from jax.experimental import pallas as pl
from jax.experimental.pallas import tpu as pltpu
from jax.sharding import PartitionSpec as P

BF16, F32 = jnp.bfloat16, jnp.float32


def even_groups(peers):
    return [[i, i + 1] for i in range(0, peers, 2)]


def odd_groups(peers, cores):
    inner = [[i * cores + c, (i + 1) * cores + c] for i in range(1, peers - 1, 2) for c in range(cores)]
    return inner + [[i * cores + c, i * cores + c + 1] for i in (0, peers - 1) for c in range(0, cores, 2)]


def swap(outward, inward):
    peers, cores = lax.axis_size("gz"), lax.axis_size("gy")
    pair = lax.ppermute(inward, "gz", [(i, i ^ 1) for i in range(peers)])
    across = lax.all_gather(outward, ("gz", "gy"), axis_index_groups=odd_groups(peers, cores))
    return pair, across


def at_end():
    gz = lax.axis_index("gz")
    return (gz == 0) | (gz == lax.axis_size("gz") - 1)


def local(body, inputs, outs, scratch=(), flops=0, kept=(), sems=0, same={}):
    vmem, kept_in_place = pl.BlockSpec(memory_space=pltpu.VMEM), pl.BlockSpec(memory_space=pltpu.HBM)
    specs = [kept_in_place if n in kept else vmem for n in range(len(inputs) + len(outs))]
    inputs = [pltpu.with_memory_space_constraint(a, pltpu.HBM) if n in kept else a for n, a in enumerate(inputs)]
    return pl.pallas_call(
        body,
        out_shape=[jax.ShapeDtypeStruct(*out) for out in outs],
        in_specs=specs[: len(inputs)],
        out_specs=specs[len(inputs) :],
        input_output_aliases=same,
        scratch_shapes=[pltpu.VMEM(*one) for one in scratch] + [pltpu.SemaphoreType.DMA((sems,))] * (sems > 0),
        cost_estimate=pl.CostEstimate(flops=flops, bytes_accessed=1 << 20, transcendentals=0),
        compiler_params=pltpu.CompilerParams(vmem_limit_bytes=32 << 20),
    )(*inputs)


def three_taps(wide, width, chans):
    cells = wide.shape[0]
    column = lax.broadcasted_iota(jnp.int32, (cells, chans), 0) % width
    left = jnp.where(column == 0, 0.0, pltpu.roll(wide[:, :chans], 1, 0))
    right = jnp.where(column == width - 1, 0.0, pltpu.roll(wide[:, 2 * chans :], cells - 1, 0))
    return left + wide[:, chans : 2 * chans] + right


TAPS = [(i, j) for i in range(3) for j in range(3)]


def edges(volume, own, outward, inward, sem):
    odd = lax.axis_index("gz") % 2
    read = pltpu.make_async_copy(volume, own, sem.at[0])
    read.start()
    read.wait()
    outward[...] = own[pl.ds(odd, 3)]
    inward[...] = own[pl.ds(1 - odd, 3)]


def stacked(kernel, axis):
    taps = [jnp.concatenate([kernel[i, j, tap] for tap in range(3)], axis=axis) for i, j in TAPS]
    return jnp.concatenate(taps, axis=1 - axis)


def join(volume, pair, across, wide, rows):
    odd, gy = lax.axis_index("gz") % 2, lax.axis_index("gy")
    wide[3:7] = volume[...]
    wide[pl.ds(7 * (1 - odd), 3)] = pair[...]
    wide[pl.ds(7 * odd, 3)] = across[odd]

    @pl.when(at_end())
    def _():
        wide[pl.ds(7 * odd, 3)] = jnp.zeros((3, 4, 32, 128), BF16)

    rows[0] = wide[:, 3 * (1 - gy % 2)]
    rows[1] = wide[:, jnp.where(gy < 2, 2, 1)]


def masked(cells, inside):
    return (cells.astype(F32) * jnp.where(inside, 1.0, 0.0)).astype(BF16)


def level_a(wide, rows, kernel, bias, skip, ship, x, most):
    gy = lax.axis_index("gy")
    core = gy % 2
    x[:, 1:5] = wide[...]
    x[:, 5 * (1 - core)] = rows[1 - core, 0]
    x[:, 5 * core] = jnp.zeros((10, 32, 128), BF16)
    open_row = jnp.where(gy == 1, 3, jnp.where(gy == 2, 0, 4))
    row = lax.broadcasted_iota(jnp.int32, (256, 128), 0) // 32 % 4
    weights = stacked(kernel, 1)
    for p in (1, 2, 0, 3):
        z = 2 * p
        cells = jnp.concatenate([x[z + i : z + i + 2, j : j + 4].reshape(256, 128) for i, j in TAPS], axis=1)
        sums = jnp.dot(cells, weights, preferred_element_type=F32)
        out = jnp.maximum(three_taps(sums, 32, 128) + bias[...], 0.0)
        if p in (1, 2):
            skip[z - 2 : z] = out.astype(BF16).reshape(2, 4, 32, 128)
        closed = jnp.where(row == open_row, 0.0, out)
        most[...] = jnp.max(closed.reshape(2, 2, 2, 32, 128), axis=(0, 2)).reshape(64, 128)
        small = jnp.maximum(most[pl.ds(0, 32, stride=2)], most[pl.ds(1, 32, stride=2)])
        ship[p] = small.astype(BF16)

    @pl.when((gy == 1) | (gy == 2))
    def _():
        ship[4:14] = wide[:, jnp.where(gy == 1, 3, 0)]

    @pl.when((gy == 0) | (gy == 3))
    def _():
        ship[4:14] = rows[1 - core, 1]


def level_b(ships, kernel_a, bias_a, kernel, bias, skip_a, patch, skip, pooled, out_a, x, most_a, most, sem):
    gz = lax.axis_index("gz")
    write = pltpu.make_async_copy(skip_a, out_a, sem.at[0])
    write.start()
    weights_a = stacked(kernel_a, 1)
    x[:, 0] = jnp.zeros((4, 16, 128), BF16)
    x[:, 9] = jnp.zeros((4, 16, 128), BF16)
    for g in range(4):
        x[:, 2 * g + 1 : 2 * g + 3] = ships[g, 0:4].reshape(4, 2, 16, 128)
    open_rows = []
    for r in range(2):
        cells = jnp.concatenate([ships[r + j, 4 + i : 12 + i].reshape(256, 128) for i, j in TAPS], axis=1)
        sums = jnp.dot(cells, weights_a, preferred_element_type=F32)
        out = jnp.maximum(three_taps(sums, 32, 128) + bias_a[...], 0.0)
        open_rows.append(out[64:192].astype(BF16).reshape(4, 32, 128))
        most_a[...] = jnp.max(out.reshape(4, 2, 32, 128), axis=1).reshape(128, 128)
        small = jnp.maximum(most_a[pl.ds(0, 64, stride=2)], most_a[pl.ds(1, 64, stride=2)])
        x[:, 4 + r] = jnp.maximum(x[:, 4 + r], small.astype(BF16).reshape(4, 16, 128))
    patch[0] = open_rows[0]
    patch[1] = open_rows[1]
    x[0] = masked(x[0], gz > 0)
    x[3] = masked(x[3], gz < lax.axis_size("gz") - 1)
    weights = stacked(kernel, 0)
    cells = jnp.concatenate([x[i : i + 2, j : j + 8].reshape(256, 128) for i, j in TAPS], axis=1)
    sums = lax.dot_general(cells, weights, (((1,), (1,)), ((), ())), preferred_element_type=F32)
    out = jnp.maximum(three_taps(sums, 16, 64) + bias[...], 0.0)
    skip[...] = out.astype(BF16).reshape(2, 8, 16, 64)
    most[...] = jnp.max(out.reshape(2, 4, 2, 16, 64), axis=(0, 2)).reshape(64, 64)
    small = jnp.maximum(most[pl.ds(0, 32, stride=2)], most[pl.ds(1, 32, stride=2)])
    pooled[...] = small.astype(BF16).reshape(1, 4, 8, 64)
    write.wait()


def level_c(own, pair, across, kernel, bias, skip_a, patch, skip_b, bottom, out_a, out_b, x, sem):
    gy, odd = lax.axis_index("gy"), lax.axis_index("gz") % 2
    write_b = pltpu.make_async_copy(skip_b, out_b, sem.at[0])
    write_b.start()
    inner = (gy == 1) | (gy == 2)
    upper = jnp.where(gy == 2, 1, 0)
    write_a = pltpu.make_async_copy(patch.at[upper], out_a.at[:, 3 * (1 - upper)], sem.at[1])

    @pl.when(inner)
    def _():
        write_a.start()

    x[:, 0] = jnp.zeros((3, 8, 256), BF16)
    x[:, 5] = jnp.zeros((3, 8, 256), BF16)
    x[1, 1:5] = jnp.concatenate([own[g] for g in range(4)], axis=-1)
    x[2 * (1 - odd), 1:5] = jnp.concatenate([pair[g] for g in range(4)], axis=-1)
    x[2 * odd, 1:5] = jnp.concatenate([across[odd, g] for g in range(4)], axis=-1)

    @pl.when(at_end())
    def _():
        x[2 * odd, 1:5] = jnp.zeros((4, 8, 256), BF16)

    weights = stacked(kernel, 1)
    cells = jnp.concatenate([x[i, j : j + 4].reshape(32, 256) for i, j in TAPS], axis=1)
    sums = jnp.dot(cells, weights, preferred_element_type=F32)
    out = jnp.maximum(three_taps(sums, 8, 128) + bias[...], 0.0)
    bottom[...] = out.astype(BF16).reshape(1, 4, 8, 128)
    write_b.wait()

    @pl.when(inner)
    def _():
        write_a.wait()


def levels(volume, kernel_a, bias_a, kernel_b, bias_b, kernel_c, bias_c):
    slab = ((3, 4, 32, 128), BF16)
    own, outward, inward = local(edges, (volume,), [((4, 4, 32, 128), BF16), slab, slab], kept=(0,), sems=1)
    pair, across = swap(outward, inward)
    joined = [((10, 4, 32, 128), BF16), ((2, 10, 32, 128), BF16)]
    wide, rows = local(join, (own, pair, across), joined, flops=1 << 33)
    rows = lax.all_gather(rows, "gy", axis_index_groups=even_groups(4))
    skip_a, ship = local(
        level_a,
        (wide, rows, kernel_a, bias_a[None]),
        [((4, 4, 32, 128), BF16), ((14, 32, 128), BF16)],
        [((10, 6, 32, 128), BF16), ((64, 128), F32)],
        1 << 30,
    )
    patch, skip_b, pooled_b, skip_a = local(
        level_b,
        (lax.all_gather(ship, "gy"), kernel_a, bias_a[None], jnp.swapaxes(kernel_b, 3, 4), bias_b[None], skip_a),
        [((2, 4, 32, 128), BF16), ((2, 8, 16, 64), BF16), ((1, 4, 8, 64), BF16), ((4, 4, 32, 128), BF16)],
        [((4, 10, 16, 128), BF16), ((128, 128), F32), ((64, 64), F32)],
        1 << 29,
        kept=(9,),
        sems=1,
    )
    channels = lax.all_gather(pooled_b, "gy", tiled=True)
    pair, across = swap(channels, channels)
    bottom, skip_a, skip_b = local(
        level_c,
        (channels, pair, across, kernel_c, bias_c[None], skip_a, patch, skip_b),
        [((1, 4, 8, 128), BF16), ((4, 4, 32, 128), BF16), ((2, 8, 16, 64), BF16)],
        [((3, 6, 8, 256), BF16)],
        1 << 27,
        kept=(5, 9, 10),
        sems=2,
        same={5: 1},
    )
    return (skip_a, skip_b, bottom)


def solution(mesh):
    return jax.shard_map(
        levels,
        mesh=mesh,
        in_specs=(
            P("gz", "gy", None, None),
            P(),
            P(),
            P(None, None, None, None, "gy"),
            P("gy"),
            P(None, None, None, None, "gy"),
            P("gy"),
        ),
        out_specs=(P("gz", "gy", None, None), P("gz", None, None, "gy"), P("gz", None, None, "gy")),
        check_vma=False,
    )
```
